32 devices in a mesh: dom: 8 (over z, y), sub: 4 (over x, core).
Axes of the slice: x: 2, y: 2, z: 4, core: 2. Of those that a mesh axis runs over, the one named last changes fastest.
Arguments:
- positions: float32 [3, 131072], P(None, ('dom', 'sub')), may hold values from -20 to 20
- mass: float32 [131072], P(('dom', 'sub')), may hold values from 3 to 6
- local_tiles: float32 [2048, 128, 128], P(('dom', 'sub')), as said below
- local_rows: int32 [2048], P(('dom', 'sub')), may hold values from 0 to 31, as said below
- local_cols: int32 [2048], P(('dom', 'sub')), may hold values from 0 to 31, as said below
- live_tiles: int32 [32], P(('dom', 'sub')), may hold values from 32 to 64, as said below
- dom_tiles: float32 [1024, 128, 128], P(('dom', 'sub')), as said below
- dom_cols: int32 [1024], P(('dom', 'sub')), may hold values from 0 to 31
- dom_slots: int32 [1024], P(('dom', 'sub')), may hold values from 0 to 255, as said below
- dom_rows: int32 [8192], P(('dom', 'sub')), may hold values from 0 to 31, as said below
- sub_tiles: float32 [1536, 128, 128], P(('dom', 'sub')), as said below
- sub_cols: int32 [1536], P(('dom', 'sub')), may hold values from 0 to 31
- sub_slots: int32 [1536], P(('dom', 'sub')), may hold values from 0 to 63, as said below
- sub_rows: int32 [2048], P(('dom', 'sub')), may hold values from 0 to 31, as said below
- precond: float32 [1024, 128, 128], P(('dom', 'sub')), may hold values from -0.05 to 0.3, as said below
Outputs:
- solution: float32 [3, 131072], P(None, ('dom', 'sub'))
- residual: float32 [3, 131072], P(None, ('dom', 'sub'))
The draws below stay inside these ranges and needn't reach their ends.
Inputs may be any that keep to these rules, and one draw needn't show every extreme that they name: Device d uses the first live_tiles[d] of its 64 interior tiles, an even number; some device uses all of them. `local_tiles`: interior tiles come in pairs 2i, 2i + 1 of a device: the second is the transpose of the first. `local_rows`: tile 2i + 1 of a device has the block row and column of tile 2i swapped. `local_cols`: tile 2i + 1 of a device has the block row and column of tile 2i swapped. `dom_slots`: the destination group of a tile differs from its device's dom index in exactly one of its 3 bits; no two tiles of a device share a slot. `dom_rows`: entries for slots that no tile fills are arbitrary blocks of the receiver. `dom_tiles`: every coupling tile that reaches block row r of a device from block column c of another has a transposed tile on the receiver, from its block column r, that reaches block row c of the sender; so A is symmetric. `sub_slots`: the destination partition of a tile lies in its device's group and is not its device's own; no two tiles of a device share a slot. `sub_rows`: entries for slots that no tile fills are arbitrary blocks of the receiver. `sub_tiles`: every such tile has a transposed partner on the receiving partition that is routed back to the sender's block column. `precond`: every block is symmetric and positive definite.
All inputs are finite; a program needn't handle non-finite values.
Results may differ from the reference program's by a relative error of at most 0.0003.
Values sent between devices are 32-bit elements; how exact they have to be, the bound alone decides.
No kernel may reach another device: no remote copies, remote signals or barrier semaphores. Data moves between devices by JAX's collectives and lax.ppermute only.
A program may use at most 64 MiB of HBM per device.

```python
import math
import jax
import jax.numpy as jnp
from jax import lax

TILE = 128
DIMS = 3
NB = 32
ITERS = 3
DBITS = 3
LT = 64
IFD = 32
IFS = 48
SD = 32
SS = 16
V_DEV = 4096
VERTS = 131072
N_DOM = 8
N_SUB = 4


def tile_noise(key, shape):
    values = jax.random.normal(key, shape, jnp.float32)
    return jnp.clip(values, -6.0, 6.0) / math.sqrt(8 * TILE)


def draw_positions(key, part):
    devices_all = VERTS // V_DEV
    owners = jnp.arange(VERTS, dtype=jnp.int32) // V_DEV
    scaling = 1.0 + 2.0 * owners.astype(jnp.float32) / max(devices_all - 1, 1)
    base = jnp.clip(jax.random.normal(key, (DIMS, VERTS), jnp.float32), -6.0, 6.0)
    return jnp.clip(base * scaling[None, :], -20.0, 20.0)


def local_plan(key):
    devices_all = VERTS // V_DEV
    subkeys = jax.random.split(jax.random.fold_in(key, 5), 3)
    first_rows = jax.random.randint(subkeys[0], (devices_all * NB,), 0, NB, dtype=jnp.int32)
    first_cols = jax.random.randint(subkeys[1], (devices_all * NB,), 0, NB, dtype=jnp.int32)
    return (first_rows, first_cols, subkeys[2])


def draw_local_tiles(key, part):
    devices_all = VERTS // V_DEV
    first_rows, first_cols, tile_key = local_plan(key)
    halves = tile_noise(tile_key, (devices_all * NB, TILE, TILE))
    paired = jnp.stack([halves, jnp.swapaxes(halves, 1, 2)], axis=1)
    return paired.reshape(devices_all * LT, TILE, TILE)


def draw_local_rows(key, part):
    first_rows, first_cols, tile_key = local_plan(key)
    return jnp.stack([first_rows, first_cols], axis=1).reshape(-1).astype(jnp.int32)


def draw_local_cols(key, part):
    first_rows, first_cols, tile_key = local_plan(key)
    return jnp.stack([first_cols, first_rows], axis=1).reshape(-1).astype(jnp.int32)


def draw_live_tiles(key, part):
    devices_all = VERTS // V_DEV
    first, second = jax.random.split(key)
    values = 2 * jax.random.randint(first, (devices_all,), NB // 2, NB + 1, dtype=jnp.int32)
    chosen = jax.random.randint(second, (), 0, devices_all, dtype=jnp.int32)
    return jnp.where(jnp.arange(devices_all, dtype=jnp.int32) == chosen, LT, values).astype(jnp.int32)


def dom_plan(key):
    devices_all = VERTS // V_DEV
    half = IFD // 2
    subkeys = jax.random.split(jax.random.fold_in(key, 11), 5)
    bit_choice = jax.random.randint(subkeys[0], (N_SUB, half), 0, DBITS, dtype=jnp.int32)
    bit_choice = bit_choice.at[0, 0].set(DBITS - 1)
    cols_up = jax.random.randint(subkeys[1], (devices_all, half), 0, NB, dtype=jnp.int32)
    rows_up = jax.random.randint(subkeys[2], (devices_all, half), 0, NB, dtype=jnp.int32)
    device_ids = jnp.arange(devices_all, dtype=jnp.int32)
    group_of = device_ids // N_SUB
    member_of = device_ids % N_SUB
    flip_dev = jnp.left_shift(jnp.ones((devices_all, half), jnp.int32), bit_choice[member_of])
    source_down = jnp.bitwise_xor(group_of[:, None], flip_dev) * N_SUB + member_of[:, None]
    return (flip_dev, cols_up, rows_up, source_down, group_of, member_of, subkeys[3], subkeys[4])


def draw_dom_tiles(key, part):
    devices_all = VERTS // V_DEV
    half = IFD // 2
    flip_dev, cols_up, rows_up, source_down, group_of, member_of, tile_key, fill_key = dom_plan(key)
    upward = tile_noise(tile_key, (devices_all, half, TILE, TILE))
    slot_ids = jnp.arange(half, dtype=jnp.int32)[None, :]
    downward = jnp.swapaxes(upward[source_down, slot_ids], 2, 3)
    return jnp.concatenate([upward, downward], axis=1).reshape(devices_all * IFD, TILE, TILE)


def draw_dom_cols(key, part):
    half = IFD // 2
    flip_dev, cols_up, rows_up, source_down, group_of, member_of, tile_key, fill_key = dom_plan(key)
    slot_ids = jnp.arange(half, dtype=jnp.int32)[None, :]
    return jnp.concatenate([cols_up, rows_up[source_down, slot_ids]], axis=1).reshape(-1).astype(jnp.int32)


def draw_dom_slots(key, part):
    half = IFD // 2
    flip_dev, cols_up, rows_up, source_down, group_of, member_of, tile_key, fill_key = dom_plan(key)
    slot_ids = jnp.arange(half, dtype=jnp.int32)[None, :]
    partner = jnp.bitwise_xor(group_of[:, None], flip_dev)
    upward = partner * SD + slot_ids
    downward = partner * SD + half + slot_ids
    return jnp.concatenate([upward, downward], axis=1).reshape(-1).astype(jnp.int32)


def draw_dom_rows(key, part):
    devices_all = VERTS // V_DEV
    half = IFD // 2
    flip_dev, cols_up, rows_up, source_down, group_of, member_of, tile_key, fill_key = dom_plan(key)
    filler = jax.random.randint(fill_key, (devices_all, N_DOM, SD), 0, NB, dtype=jnp.int32)
    groups = jnp.arange(N_DOM, dtype=jnp.int32)[None, :, None]
    mine = group_of[:, None, None]
    flip_full = jnp.concatenate([flip_dev, flip_dev], axis=1)[:, None, :]
    slots = jnp.arange(SD, dtype=jnp.int32)[None, None, :]
    is_down = slots >= half
    slot_mod = slots % half
    matched = jnp.bitwise_xor(groups, flip_full) == mine
    sender = groups * N_SUB + member_of[:, None, None]
    up_value = rows_up[sender, slot_mod]
    own = jnp.arange(devices_all, dtype=jnp.int32)[:, None, None]
    down_value = cols_up[own, slot_mod]
    result = jnp.where(matched, jnp.where(is_down, down_value, up_value), filler)
    return result.reshape(-1).astype(jnp.int32)


def sub_plan(key):
    devices_all = VERTS // V_DEV
    half = IFS // 2
    subkeys = jax.random.split(jax.random.fold_in(key, 23), 5)
    turn = jax.random.randint(subkeys[0], (N_DOM,), 0, N_SUB - 1, dtype=jnp.int32)
    cols_up = jax.random.randint(subkeys[1], (devices_all, half), 0, NB, dtype=jnp.int32)
    rows_up = jax.random.randint(subkeys[2], (devices_all, half), 0, NB, dtype=jnp.int32)
    device_ids = jnp.arange(devices_all, dtype=jnp.int32)
    group_of = device_ids // N_SUB
    member_of = device_ids % N_SUB
    slot_ids = jnp.arange(half, dtype=jnp.int32)[None, :]
    offset_dev = 1 + (slot_ids + turn[group_of][:, None]) % (N_SUB - 1)
    level = slot_ids // (N_SUB - 1)
    source_down = group_of[:, None] * N_SUB + (member_of[:, None] - offset_dev) % N_SUB
    return (turn, cols_up, rows_up, offset_dev, level, source_down, group_of, member_of, subkeys[3], subkeys[4])


def draw_sub_tiles(key, part):
    devices_all = VERTS // V_DEV
    half = IFS // 2
    turn, cols_up, rows_up, offset_dev, level, source_down, group_of, member_of, tile_key, fill_key = sub_plan(key)
    upward = tile_noise(tile_key, (devices_all, half, TILE, TILE))
    slot_ids = jnp.arange(half, dtype=jnp.int32)[None, :]
    downward = jnp.swapaxes(upward[source_down, slot_ids], 2, 3)
    return jnp.concatenate([upward, downward], axis=1).reshape(devices_all * IFS, TILE, TILE)


def draw_sub_cols(key, part):
    half = IFS // 2
    turn, cols_up, rows_up, offset_dev, level, source_down, group_of, member_of, tile_key, fill_key = sub_plan(key)
    slot_ids = jnp.arange(half, dtype=jnp.int32)[None, :]
    return jnp.concatenate([cols_up, rows_up[source_down, slot_ids]], axis=1).reshape(-1).astype(jnp.int32)


def draw_sub_slots(key, part):
    turn, cols_up, rows_up, offset_dev, level, source_down, group_of, member_of, tile_key, fill_key = sub_plan(key)
    upward = (member_of[:, None] + offset_dev) % N_SUB * SS + level
    downward = (member_of[:, None] - offset_dev) % N_SUB * SS + SS // 2 + level
    return jnp.concatenate([upward, downward], axis=1).reshape(-1).astype(jnp.int32)


def draw_sub_rows(key, part):
    devices_all = VERTS // V_DEV
    half = IFS // 2
    half_slots = SS // 2
    turn, cols_up, rows_up, offset_dev, level, source_down, group_of, member_of, tile_key, fill_key = sub_plan(key)
    filler = jax.random.randint(fill_key, (devices_all, N_SUB, SS), 0, NB, dtype=jnp.int32)
    others = jnp.arange(N_SUB, dtype=jnp.int32)[None, :, None]
    mine = member_of[:, None, None]
    group_here = group_of[:, None, None]
    slots = jnp.arange(SS, dtype=jnp.int32)[None, None, :]
    is_down = slots >= half_slots
    depth = jnp.where(is_down, slots - half_slots, slots)
    needed = jnp.where(is_down, (others - mine) % N_SUB, (mine - others) % N_SUB)
    rest = (needed - 1 - turn[group_of][:, None, None]) % (N_SUB - 1)
    index = depth * (N_SUB - 1) + rest
    valid = (needed != 0) & (index < half)
    safe = jnp.clip(index, 0, half - 1)
    sender = group_here * N_SUB + others
    up_value = rows_up[sender, safe]
    own = jnp.broadcast_to(jnp.arange(devices_all, dtype=jnp.int32)[:, None, None], (devices_all, N_SUB, SS))
    down_value = cols_up[own, safe]
    chosen = jnp.where(is_down, down_value, up_value)
    return jnp.where(valid, chosen, filler).reshape(-1).astype(jnp.int32)


def draw_precond(key, part):
    total = VERTS // TILE
    first, second = jax.random.split(key)
    noise = jax.random.normal(first, (total, TILE, TILE), jnp.float32) * (0.045 / math.sqrt(TILE))
    noise = jnp.clip((noise + jnp.swapaxes(noise, 1, 2)) * 0.7071, -0.05, 0.05)
    diagonal = jax.random.uniform(second, (total, TILE), jnp.float32, 0.12, 0.3)
    identity_tile = jnp.eye(TILE, dtype=jnp.float32)
    return noise * (1.0 - identity_tile) + identity_tile * diagonal[:, :, None]


def shard_levels(rng, dims, shards, smallest, largest):
    level, own = 1.0, jax.random.fold_in(rng, 6)
    for dim, blocks in shards:
        steps = jnp.exp(jax.random.uniform(jax.random.fold_in(own, dim), (blocks,), jnp.float32, smallest / len(shards), largest / len(shards)))
        level = level * jnp.repeat(steps, dims[dim] // blocks).reshape([-1 if axis == dim else 1 for axis in range(len(dims))])
    return level


def setup_inputs(seed: int = 0) -> dict:
    streams_of = jax.random.split(jax.random.key(seed), 16)
    return {
        "positions": draw_positions(jax.random.fold_in(streams_of[15], 71), 0),
        "mass": jnp.clip(3.0 + 3.0 * jax.random.uniform(streams_of[1], (VERTS,), jnp.float32) ** shard_levels(streams_of[1], (VERTS,), ((0, 32),), -0.2, 0.2), 3.0, 6.0),
        "local_tiles": draw_local_tiles(jax.random.fold_in(streams_of[15], 71), 0),
        "local_rows": draw_local_rows(jax.random.fold_in(streams_of[15], 71), 0),
        "local_cols": draw_local_cols(jax.random.fold_in(streams_of[15], 71), 0),
        "live_tiles": draw_live_tiles(jax.random.fold_in(streams_of[15], 71), 0),
        "dom_tiles": draw_dom_tiles(jax.random.fold_in(streams_of[15], 71), 0),
        "dom_cols": draw_dom_cols(jax.random.fold_in(streams_of[15], 71), 0),
        "dom_slots": draw_dom_slots(jax.random.fold_in(streams_of[15], 71), 0),
        "dom_rows": draw_dom_rows(jax.random.fold_in(streams_of[15], 71), 0),
        "sub_tiles": draw_sub_tiles(jax.random.fold_in(streams_of[15], 71), 0),
        "sub_cols": draw_sub_cols(jax.random.fold_in(streams_of[15], 71), 0),
        "sub_slots": draw_sub_slots(jax.random.fold_in(streams_of[15], 71), 0),
        "sub_rows": draw_sub_rows(jax.random.fold_in(streams_of[15], 71), 0),
        "precond": draw_precond(jax.random.fold_in(streams_of[15], 71), 0),
    }


PRECISE = lax.Precision.HIGHEST


def tile_terms(tile_stack, columns, blocks, devices_all):
    per_device = tile_stack.shape[0] // devices_all
    owners = jnp.arange(tile_stack.shape[0], dtype=jnp.int32) // per_device
    picked = jnp.take(blocks, owners * NB + columns, axis=1)
    products = jnp.einsum("tij,ktj->tki", tile_stack, picked, precision=PRECISE)
    return products, owners, per_device


def apply_operator(vector, mass, local_tiles, local_rows, local_cols, live_tiles, dom_tiles, dom_cols, dom_slots, dom_rows, sub_tiles, sub_cols, sub_slots, sub_rows):
    devices_all = VERTS // V_DEV
    components = vector.shape[0]
    blocks = vector.reshape(components, devices_all * NB, TILE)
    products, owners, per_device = tile_terms(local_tiles, local_cols, blocks, devices_all)
    place_in = jnp.arange(local_tiles.shape[0], dtype=jnp.int32) - owners * per_device
    live_mask = (place_in < live_tiles[owners]).astype(vector.dtype)
    summed = jax.ops.segment_sum(products * live_mask[:, None, None], owners * NB + local_rows, num_segments=devices_all * NB)
    products, owners, per_device = tile_terms(dom_tiles, dom_cols, blocks, devices_all)
    outgoing = jax.ops.segment_sum(products, owners * (N_DOM * SD) + dom_slots, num_segments=devices_all * N_DOM * SD)
    outgoing = outgoing.reshape(N_DOM, N_SUB, N_DOM, SD, components, TILE).transpose(2, 1, 0, 3, 4, 5)
    outgoing = outgoing.reshape(devices_all * N_DOM * SD, components, TILE)
    receivers = jnp.arange(devices_all * N_DOM * SD, dtype=jnp.int32) // (N_DOM * SD)
    summed = summed + jax.ops.segment_sum(outgoing, receivers * NB + dom_rows, num_segments=devices_all * NB)
    products, owners, per_device = tile_terms(sub_tiles, sub_cols, blocks, devices_all)
    outgoing = jax.ops.segment_sum(products, owners * (N_SUB * SS) + sub_slots, num_segments=devices_all * N_SUB * SS)
    outgoing = outgoing.reshape(N_DOM, N_SUB, N_SUB, SS, components, TILE).transpose(0, 2, 1, 3, 4, 5)
    outgoing = outgoing.reshape(devices_all * N_SUB * SS, components, TILE)
    receivers = jnp.arange(devices_all * N_SUB * SS, dtype=jnp.int32) // (N_SUB * SS)
    summed = summed + jax.ops.segment_sum(outgoing, receivers * NB + sub_rows, num_segments=devices_all * NB)
    return mass[None, :] * vector + summed.transpose(1, 0, 2).reshape(components, VERTS)


def apply_precond(vector, precond):
    components = vector.shape[0]
    blocks = vector.reshape(components, VERTS // TILE, TILE)
    return jnp.einsum("bij,kbj->kbi", precond, blocks, precision=PRECISE).reshape(components, VERTS)


def reference(positions, mass, local_tiles, local_rows, local_cols, live_tiles, dom_tiles, dom_cols, dom_slots, dom_rows, sub_tiles, sub_cols, sub_slots, sub_rows, precond):
    def operate(vector):
        return apply_operator(vector, mass, local_tiles, local_rows, local_cols, live_tiles, dom_tiles, dom_cols, dom_slots, dom_rows, sub_tiles, sub_cols, sub_slots, sub_rows)

    solution = positions
    residual = mass[None, :] * positions - operate(positions)
    smoothed = apply_precond(residual, precond)
    direction = smoothed
    current = jnp.sum(residual * smoothed, axis=1)
    for iteration in range(ITERS):
        applied = operate(direction)
        step_size = current / jnp.sum(direction * applied, axis=1)
        solution = solution + step_size[:, None] * direction
        residual = residual - step_size[:, None] * applied
        if iteration + 1 < ITERS:
            smoothed = apply_precond(residual, precond)
            following = jnp.sum(residual * smoothed, axis=1)
            direction = smoothed + (following / current)[:, None] * direction
            current = following
    return solution, residual
```

```python
import math

import jax
import jax.numpy as jnp
from jax import lax
from jax.experimental import pallas as pl
from jax.experimental.pallas import tpu as pltpu
from jax.sharding import PartitionSpec as P

ITERS = 3
SHIFT = 1.0
F32 = jnp.float32
BF16 = jnp.bfloat16


VMEM = pl.BlockSpec(memory_space=pltpu.VMEM)
SMEM = pl.BlockSpec(memory_space=pltpu.SMEM)
ANY = pl.BlockSpec(memory_space=pl.ANY)


def pair_dot(left_a, left_b, tile_a, tile_b):
    lhs = jnp.concatenate([left_a, left_b], axis=0).astype(BF16)
    lhs = jnp.concatenate([lhs, lhs], axis=1)
    both = jnp.concatenate([tile_a, tile_b], axis=1)
    high = both.astype(BF16)
    low = (both - high.astype(F32)).astype(BF16)
    out = jnp.dot(lhs, jnp.concatenate([high, low], axis=0), preferred_element_type=F32)
    size = tile_a.shape[1]
    return out[0:8, 0:size], out[8:16, size : 2 * size]


def put_rows(rows_ref, start, planes):
    components = len(planes)
    count = planes[0].shape[0]
    for k, plane in enumerate(planes):
        high = plane.astype(BF16).astype(F32)
        rows_ref[pl.ds(start * 8 + k, count, stride=8), :] = high
        rows_ref[pl.ds(start * 8 + components + k, count, stride=8), :] = plane - high
    for k in range(2 * components, 8):
        rows_ref[pl.ds(start * 8 + k, count, stride=8), :] = jnp.zeros(planes[0].shape, F32)


def take_rows(rows_ref, components, count):
    return [
        rows_ref[pl.ds(k, count, stride=8), :] + rows_ref[pl.ds(components + k, count, stride=8), :]
        for k in range(components)
    ]


def rows_at(ref, index):
    return ref[pl.ds(pl.multiple_of(index * 8, 8), 8), :]


def make_calls(shape):
    nb, size, comps = shape["nb"], shape["size"], shape["comps"]
    lt, ifd, ifs = shape["lt"], shape["ifd"], shape["ifs"]
    sd, ss, bits, turns = shape["sd"], shape["ss"], shape["bits"], shape["turns"]
    field = jax.ShapeDtypeStruct((comps, nb, size), F32)
    sends = [jax.ShapeDtypeStruct((comps, sd, size), F32)] * bits
    sends += [jax.ShapeDtypeStruct((comps, ss, size), F32)] * turns
    slots = bits * sd + turns * ss
    remote = ifd + ifs
    at_rows, at_cols = 0, lt
    at_src = 2 * lt
    at_rcol = at_src + remote
    at_send = at_rcol + remote
    at_live = at_send + slots
    chunk = math.gcd(math.gcd(lt, ifd), math.gcd(math.gcd(ifs, nb), 8))

    def write_sends(table, v_ref, outs):
        base = at_send
        for out in outs:
            for s in range(out.shape[1]):
                row = table[base + s]
                for k in range(comps):
                    out[k, pl.ds(s, 1), :] = v_ref[k, pl.ds(row, 1), :]
            base += out.shape[1]

    def send_kernel(table, v_ref, *outs):
        write_sends(table, v_ref, outs)

    def local_kernel(table, v_ref, tiles_hbm, acc_ref, tiles, rows_ref, sems):
        copies = [
            pltpu.make_async_copy(
                tiles_hbm.at[pl.ds(c * chunk, chunk)], tiles.at[pl.ds(c * chunk, chunk)], sems.at[c]
            )
            for c in range(lt // chunk)
        ]
        for copy in copies:
            copy.start()
        put_rows(rows_ref, 0, [v_ref[k] for k in range(comps)])
        acc_ref[...] = jnp.zeros(acc_ref.shape, F32)

        def step(c, carry):
            pltpu.make_async_copy(
                tiles_hbm.at[pl.ds(c * chunk, chunk)], tiles.at[pl.ds(c * chunk, chunk)], sems.at[c]
            ).wait()
            results = []
            for j in range(0, chunk, 2):
                t = c * chunk + j
                results.extend(
                    pair_dot(
                        rows_at(rows_ref, table[at_rows + t]),
                        rows_at(rows_ref, table[at_rows + t + 1]),
                        tiles[t],
                        tiles[t + 1],
                    )
                )
            for j in range(chunk):
                t = c * chunk + j
                live = t < table[at_live]
                place = pl.ds(pl.multiple_of(table[at_cols + t] * 8, 8), 8)
                acc_ref[place, :] += jnp.where(live, results[j], 0.0)
            return carry

        lax.fori_loop(0, lt // chunk, step, 0)

    def remote_kernel(first, last, table, v_ref, mass_ref, local_acc, *refs):
        arrived, refs = refs[: bits + turns], refs[bits + turns :]
        dom_hbm, sub_hbm, refs = refs[0], refs[1], refs[2:]
        if not last:
            pre_hbm, w_ref, z_ref, refs = refs[0], refs[1], refs[2], refs[3:]
            outs, refs = refs[: bits + turns], refs[bits + turns :]
            sources = ((dom_hbm, ifd), (sub_hbm, ifs), (pre_hbm, nb))
        else:
            past, refs = refs[: 2 * ITERS], refs[2 * ITERS :]
            w_ref, gram_ref, refs = refs[0], refs[1], refs[2:]
            sources = ((dom_hbm, ifd), (sub_hbm, ifs))
        tiles, rows_ref, acc_ref, sems = refs
        base = 0
        for source, count in sources:
            for c in range(count // chunk):
                pltpu.make_async_copy(
                    source.at[pl.ds(c * chunk, chunk)],
                    tiles.at[pl.ds(base + c * chunk, chunk)],
                    sems.at[(base // chunk) + c],
                ).start()
            base += count
        acc_ref[...] = local_acc[...]
        start = 0
        for ref in arrived:
            put_rows(rows_ref, start, [ref[k] for k in range(comps)])
            start += ref.shape[1]

        def wait_for(c):
            pltpu.make_async_copy(
                dom_hbm.at[pl.ds(0, chunk)], tiles.at[pl.ds(c * chunk, chunk)], sems.at[c]
            ).wait()

        def step(c, carry):
            wait_for(c)
            results = []
            for j in range(0, chunk, 2):
                t = c * chunk + j
                results.extend(
                    pair_dot(
                        rows_at(rows_ref, table[at_src + t]),
                        rows_at(rows_ref, table[at_src + t + 1]),
                        tiles[t],
                        tiles[t + 1],
                    )
                )
            for j in range(chunk):
                place = pl.ds(pl.multiple_of(table[at_rcol + c * chunk + j] * 8, 8), 8)
                acc_ref[place, :] += results[j]
            return carry

        lax.fori_loop(0, remote // chunk, step, 0)
        summed = take_rows(acc_ref, comps, nb)
        if first:
            applied = [-x for x in summed]
        else:
            applied = [mass_ref[...] * v_ref[k] + summed[k] for k in range(comps)]
        for k in range(comps):
            w_ref[k] = applied[k]
        if last:
            start_res, zs, ws = past[0], past[1:4], past[4:6]
            products = [(zs[i], start_res) for i in range(ITERS)]
            products += [(zs[0], ws[0]), (zs[1], ws[0]), (zs[2], ws[0])]
            products += [(zs[1], ws[1]), (zs[2], ws[1]), (zs[2], w_ref)]
            lanes = []
            for left, right in products:
                for k in range(comps):
                    lanes.append(jnp.sum(left[k] * right[k], axis=0, keepdims=True))
            while len(lanes) < 32:
                lanes.append(jnp.zeros((1, size), F32))
            quarter = lax.broadcasted_iota(jnp.int32, (8, size), 1) // 32
            folded = jnp.zeros((8, size), F32)
            for q in range(4):
                part = jnp.concatenate(lanes[q * 8 : q * 8 + 8], axis=0)
                part = part + pltpu.roll(part, 64, 1)
                part = part + pltpu.roll(part, 32, 1)
                folded = jnp.where(quarter == q, part, folded)
            gram_ref[...] = folded
            return
        put_rows(rows_ref, 0, applied)

        def pre_step(c, carry):
            wait_for(remote // chunk + c)
            results = []
            for j in range(0, chunk, 2):
                n = c * chunk + j
                results.extend(
                    pair_dot(
                        rows_at(rows_ref, n),
                        rows_at(rows_ref, n + 1),
                        tiles[remote + n],
                        tiles[remote + n + 1],
                    )
                )
            for j in range(chunk):
                acc_ref[pl.ds(pl.multiple_of((c * chunk + j) * 8, 8), 8), :] = results[j]
            return carry

        lax.fori_loop(0, nb // chunk, pre_step, 0)
        smoothed = take_rows(acc_ref, comps, nb)
        for k in range(comps):
            z_ref[k] = smoothed[k] if first else smoothed[k] - SHIFT * v_ref[k]
        write_sends(table, z_ref, outs)

    def finish_kernel(count, *refs):
        parts, refs = refs[:count], refs[count:]
        x_ref, r_ref, z0, z1, z2, w0, w1, w2, sol_ref, res_ref = refs
        total = parts[0][...]
        for part in parts[1:]:
            total = total + part[...]
        quarter = lax.broadcasted_iota(jnp.int32, (8, size), 1) // 32
        sums = [
            jnp.sum(jnp.where(quarter == q, total, 0.0), axis=1, keepdims=True) for q in range(4)
        ]

        def entry(p, k):
            m = p * comps + k
            return sums[m // 8][m % 8 : m % 8 + 1, :]

        for k in range(comps):
            g0, g1, g2, a00, a01, a02, a11, a12, a22 = [entry(p, k) for p in range(9)]
            l1 = a01 / a00
            l2 = a02 / a00
            d1 = a11 - l1 * a01
            e = a12 - l1 * a02
            m2 = e / d1
            d2 = a22 - l2 * a02 - m2 * e
            y1 = g1 - l1 * g0
            y2 = g2 - l2 * g0 - m2 * y1
            c2 = y2 / d2
            c1 = y1 / d1 - m2 * c2
            c0 = g0 / a00 - l1 * c1 - l2 * c2
            sol_ref[k] = x_ref[k] + c0 * z0[k] + c1 * z1[k] + c2 * z2[k]
            res_ref[k] = r_ref[k] - c0 * w0[k] - c1 * w1[k] - c2 * w2[k]

    acc = jax.ShapeDtypeStruct((nb * 8, size), F32)
    send_call = pl.pallas_call(
        send_kernel, out_shape=sends, in_specs=[SMEM, VMEM], out_specs=[VMEM] * len(sends)
    )
    local_call = pl.pallas_call(
        local_kernel,
        out_shape=acc,
        in_specs=[SMEM, VMEM, ANY],
        out_specs=VMEM,
        scratch_shapes=[
            pltpu.VMEM((lt, size, size), F32),
            pltpu.VMEM((nb * 8, size), F32),
            pltpu.SemaphoreType.DMA((lt // chunk,)),
        ],
    )

    def remote_call(first, last):
        held = remote if last else remote + nb
        specs = [SMEM, VMEM, VMEM, VMEM] + [VMEM] * len(sends) + [ANY, ANY]
        if last:
            specs += [VMEM] * (2 * ITERS)
            outs = [field, jax.ShapeDtypeStruct((8, size), F32)]
        else:
            specs += [ANY]
            outs = [field, field] + sends
        return pl.pallas_call(
            lambda *refs: remote_kernel(first, last, *refs),
            out_shape=outs,
            in_specs=specs,
            out_specs=[VMEM] * len(outs),
            scratch_shapes=[
                pltpu.VMEM((held, size, size), F32),
                pltpu.VMEM((max(slots, nb) * 8, size), F32),
                pltpu.VMEM((nb * 8, size), F32),
                pltpu.SemaphoreType.DMA((held // chunk,)),
            ],
        )

    def finish_call(count):
        return pl.pallas_call(
            lambda *refs: finish_kernel(count, *refs),
            out_shape=[field, field],
            in_specs=[VMEM] * (count + 8),
            out_specs=[VMEM, VMEM],
        )

    return send_call, local_call, remote_call, finish_call


def on_device(
    positions,
    mass,
    local_tiles,
    local_rows,
    local_cols,
    live_tiles,
    dom_tiles,
    dom_cols,
    dom_slots,
    dom_rows,
    sub_tiles,
    sub_cols,
    sub_slots,
    sub_rows,
    precond,
):
    count_dom = lax.axis_size("dom")
    count_sub = lax.axis_size("sub")
    nb, size = precond.shape[0], precond.shape[1]
    comps = positions.shape[0]
    sd = dom_rows.shape[0] // count_dom
    ss = sub_rows.shape[0] // count_sub
    bits = (count_dom - 1).bit_length()
    turns = count_sub - 1
    send_call, local_call, remote_call, finish_call = make_calls(
        dict(
            nb=nb,
            size=size,
            comps=comps,
            lt=local_tiles.shape[0],
            ifd=dom_tiles.shape[0],
            ifs=sub_tiles.shape[0],
            sd=sd,
            ss=ss,
            bits=bits,
            turns=turns,
        )
    )
    mine_dom = lax.axis_index("dom")
    mine_sub = lax.axis_index("sub")
    flipped = jnp.bitwise_xor(dom_slots // sd, mine_dom)
    which = sum((flipped >= (1 << j)).astype(jnp.int32) for j in range(1, bits))
    dom_src = which * sd + dom_slots % sd
    behind = (mine_sub - sub_slots // ss + count_sub) % count_sub
    sub_src = bits * sd + (behind - 1) * ss + sub_slots % ss
    send_dom = [
        lax.dynamic_slice(dom_rows, (jnp.bitwise_xor(mine_dom, 1 << j) * sd,), (sd,))
        for j in range(bits)
    ]
    send_sub = [
        lax.dynamic_slice(sub_rows, ((mine_sub + o) % count_sub * ss,), (ss,))
        for o in range(1, count_sub)
    ]
    table = jnp.concatenate(
        [local_rows, local_cols, dom_src, sub_src, dom_cols, sub_cols]
        + send_dom
        + send_sub
        + [live_tiles]
    )
    dom_pairs = [[(a, a ^ (1 << j)) for a in range(count_dom)] for j in range(bits)]
    sub_pairs = [[(b, (b + o) % count_sub) for b in range(count_sub)] for o in range(1, count_sub)]

    def exchange(sends):
        moved = [lax.ppermute(sends[j], "dom", dom_pairs[j]) for j in range(bits)]
        moved += [lax.ppermute(sends[bits + o], "sub", sub_pairs[o]) for o in range(turns)]
        return moved

    x = positions.reshape(comps, nb, size)
    weights = mass.reshape(nb, size)
    sends = send_call(table, x)
    v = x
    zs, ws = [], []
    for phase in range(ITERS + 1):
        arrived = exchange(sends)
        acc = local_call(table, v, local_tiles)
        first, last = phase == 0, phase == ITERS
        if not last:
            w, z, *sends = remote_call(first, last)(
                table, v, weights, acc, *arrived, dom_tiles, sub_tiles, precond
            )
            ws.append(w)
            zs.append(z)
            v = z
        else:
            w, gram = remote_call(first, last)(
                table, v, weights, acc, *arrived, dom_tiles, sub_tiles, ws[0], *zs, *ws[1:]
            )
            ws.append(w)
    dom_all = [[(a, (a + o) % count_dom) for a in range(count_dom)] for o in range(1, count_dom)]
    gram = sum([lax.ppermute(gram, "sub", pairs) for pairs in sub_pairs], gram)
    parts = [gram] + [lax.ppermute(gram, "dom", pairs) for pairs in dom_all]
    sol, res = finish_call(len(parts))(*parts, x, ws[0], *zs, *ws[1:])
    return sol.reshape(positions.shape), res.reshape(positions.shape)


def solution(mesh):
    both = ("dom", "sub")
    flat, tiles = P(both), P(both, None, None)
    placed = (
        P(None, both),
        flat,
        tiles,
        flat,
        flat,
        flat,
        tiles,
        flat,
        flat,
        flat,
        tiles,
        flat,
        flat,
        flat,
        tiles,
    )
    return jax.shard_map(
        on_device,
        mesh=mesh,
        in_specs=placed,
        out_specs=(P(None, both), P(None, both)),
        check_vma=False,
    )
```

```python
import math

import jax
import jax.numpy as jnp
from jax import lax
from jax.experimental import pallas as pl
from jax.experimental.pallas import tpu as pltpu
from jax.sharding import PartitionSpec as P

ITERS = 3
SHIFT = 1.0
F32 = jnp.float32
BF16 = jnp.bfloat16


VMEM = pl.BlockSpec(memory_space=pltpu.VMEM)
SMEM = pl.BlockSpec(memory_space=pltpu.SMEM)
ANY = pl.BlockSpec(memory_space=pl.ANY)


def pair_dot(left_a, left_b, tile_a, tile_b):
    lhs = jnp.concatenate([left_a, left_b], axis=0).astype(BF16)
    lhs = jnp.concatenate([lhs, lhs], axis=1)
    both = jnp.concatenate([tile_a, tile_b], axis=1)
    high = both.astype(BF16)
    low = (both - high.astype(F32)).astype(BF16)
    out = jnp.dot(lhs, jnp.concatenate([high, low], axis=0), preferred_element_type=F32)
    size = tile_a.shape[1]
    return out[0:8, 0:size], out[8:16, size : 2 * size]


def put_rows(rows_ref, start, planes):
    components = len(planes)
    count = planes[0].shape[0]
    for k, plane in enumerate(planes):
        high = plane.astype(BF16).astype(F32)
        rows_ref[pl.ds(start * 8 + k, count, stride=8), :] = high
        rows_ref[pl.ds(start * 8 + components + k, count, stride=8), :] = plane - high
    for k in range(2 * components, 8):
        rows_ref[pl.ds(start * 8 + k, count, stride=8), :] = jnp.zeros(planes[0].shape, F32)


def take_rows(rows_ref, components, count):
    return [
        rows_ref[pl.ds(k, count, stride=8), :] + rows_ref[pl.ds(components + k, count, stride=8), :]
        for k in range(components)
    ]


def rows_at(ref, index):
    return ref[pl.ds(pl.multiple_of(index * 8, 8), 8), :]


def make_calls(shape):
    nb, size, comps = shape["nb"], shape["size"], shape["comps"]
    lt, ifd, ifs = shape["lt"], shape["ifd"], shape["ifs"]
    sd, ss, bits, turns = shape["sd"], shape["ss"], shape["bits"], shape["turns"]
    field = jax.ShapeDtypeStruct((comps, nb, size), F32)
    sends = [jax.ShapeDtypeStruct((comps, sd, size), F32)] * bits
    sends += [jax.ShapeDtypeStruct((comps, ss, size), F32)] * turns
    slots = bits * sd + turns * ss
    remote = ifd + ifs
    width = bits * sd

    def dom_source(slot, mine):
        flipped = (slot // sd) ^ mine
        which = sum((flipped >= (1 << j)).astype(jnp.int32) for j in range(1, bits))
        return which * sd + slot % sd

    def sub_source(slot, mine):
        behind = (mine - slot // ss + turns + 1) % (turns + 1)
        return width + (behind - 1) * ss + slot % ss

    chunk = math.gcd(math.gcd(lt, ifd), math.gcd(math.gcd(ifs, nb), 16))

    def write_sends(dom_rows, sub_rows, v_ref, outs):
        mine_dom, mine_sub = lax.axis_index("dom"), lax.axis_index("sub")
        for j, out in enumerate(outs):
            if j < bits:
                rows, base = dom_rows, (mine_dom ^ (1 << j)) * sd
            else:
                rows, base = sub_rows, (mine_sub + (j - bits + 1)) % (turns + 1) * ss
            for s in range(out.shape[1]):
                row = rows[base + s]
                for k in range(comps):
                    out[k, pl.ds(s, 1), :] = v_ref[k, pl.ds(row, 1), :]

    def send_kernel(dom_rows, sub_rows, x_ref, v_ref, *outs):
        for n in range(nb):
            block = x_ref[:, n * size : (n + 1) * size]
            for k in range(comps):
                v_ref[k, n : n + 1, :] = block[k : k + 1]
        write_sends(dom_rows, sub_rows, v_ref, outs)

    def local_kernel(rows, cols, live, v_hbm, tiles_hbm, acc_ref, v_ref, tiles, rows_ref, sems, v_sem):
        v_copy = pltpu.make_async_copy(v_hbm, v_ref, v_sem)
        v_copy.start()
        copies = [
            pltpu.make_async_copy(
                tiles_hbm.at[pl.ds(c * chunk, chunk)], tiles.at[pl.ds(c * chunk, chunk)], sems.at[c]
            )
            for c in range(lt // chunk)
        ]
        for copy in copies:
            copy.start()
        v_copy.wait()
        put_rows(rows_ref, 0, [v_ref[k] for k in range(comps)])
        acc_ref[...] = jnp.zeros(acc_ref.shape, F32)

        def step(c, carry):
            pltpu.make_async_copy(
                tiles_hbm.at[pl.ds(c * chunk, chunk)], tiles.at[pl.ds(c * chunk, chunk)], sems.at[c]
            ).wait()
            results = []
            for j in range(0, chunk, 2):
                t = c * chunk + j
                results.extend(
                    pair_dot(
                        rows_at(rows_ref, rows[t]),
                        rows_at(rows_ref, rows[t + 1]),
                        tiles[t],
                        tiles[t + 1],
                    )
                )
            for j in range(chunk):
                t = c * chunk + j
                used = t < live[0]
                place = pl.ds(pl.multiple_of(cols[t] * 8, 8), 8)
                acc_ref[place, :] += jnp.where(used, results[j], 0.0)
            return carry

        lax.fori_loop(0, lt // chunk, step, 0)

    def remote_kernel(first, last, *refs):
        dom_slots, dom_cols, sub_slots, sub_cols, dom_rows, sub_rows = refs[:6]
        v_hbm, mass_hbm, acc_hbm = refs[6:9]
        refs = refs[9:]
        arrived, refs = refs[: bits + turns], refs[bits + turns :]
        dom_hbm, sub_hbm, refs = refs[0], refs[1], refs[2:]
        if not last:
            pre_hbm, w_ref, z_ref, refs = refs[0], refs[1], refs[2], refs[3:]
            outs, refs = refs[: bits + turns], refs[bits + turns :]
            sources = ((dom_hbm, ifd), (sub_hbm, ifs), (pre_hbm, nb))
        else:
            past, refs = refs[: 2 * ITERS], refs[2 * ITERS :]
            w_ref, gram_ref, refs = refs[0], refs[1], refs[2:]
            sources = ((dom_hbm, ifd), (sub_hbm, ifs))
        tiles, rows_ref, acc_ref, v_ref, mass_ref, got_dom, got_sub, sems, in_sems = refs
        got = [got_dom.at[j] for j in range(bits)] + [got_sub.at[o] for o in range(turns)]
        moves = list(zip(arrived, got)) + [(acc_hbm, acc_ref), (v_hbm, v_ref), (mass_hbm, mass_ref)]
        copies = [pltpu.make_async_copy(*pair, in_sems.at[i]) for i, pair in enumerate(moves)]
        for copy in copies[: len(got)]:
            copy.start()
        base = 0
        for source, count in sources:
            for c in range(count // chunk):
                pltpu.make_async_copy(
                    source.at[pl.ds(c * chunk, chunk)],
                    tiles.at[pl.ds(base + c * chunk, chunk)],
                    sems.at[(base // chunk) + c],
                ).start()
                if base == 0 and c == 0:
                    for copy in copies[len(got) :]:
                        copy.start()
            base += count
        start = 0
        for copy, ref in zip(copies, got):
            copy.wait()
            put_rows(rows_ref, start, [ref[k] for k in range(comps)])
            start += ref.shape[1]
        for copy in copies[len(got) :]:
            copy.wait()

        def wait_for(c):
            pltpu.make_async_copy(
                dom_hbm.at[pl.ds(0, chunk)], tiles.at[pl.ds(c * chunk, chunk)], sems.at[c]
            ).wait()

        def apply_tiles(base, count, slots_ref, cols_ref, source, mine):
            def step(c, carry):
                wait_for(base // chunk + c)
                results = []
                for j in range(0, chunk, 2):
                    t = c * chunk + j
                    results.extend(
                        pair_dot(
                            rows_at(rows_ref, source(slots_ref[t], mine)),
                            rows_at(rows_ref, source(slots_ref[t + 1], mine)),
                            tiles[base + t],
                            tiles[base + t + 1],
                        )
                    )
                for j in range(chunk):
                    place = pl.ds(pl.multiple_of(cols_ref[c * chunk + j] * 8, 8), 8)
                    acc_ref[place, :] += results[j]
                return carry

            lax.fori_loop(0, count // chunk, step, 0)

        apply_tiles(0, ifd, dom_slots, dom_cols, dom_source, lax.axis_index("dom"))
        apply_tiles(ifd, ifs, sub_slots, sub_cols, sub_source, lax.axis_index("sub"))
        summed = take_rows(acc_ref, comps, nb)
        if first:
            applied = [-x for x in summed]
        else:
            applied = [mass_ref[...] * v_ref[k] + summed[k] for k in range(comps)]
        for k in range(comps):
            w_ref[k] = applied[k]
        if last:
            start_res, zs, ws = past[0], past[1:4], past[4:6]
            products = [(zs[i], start_res) for i in range(ITERS)]
            products += [(zs[0], ws[0]), (zs[1], ws[0]), (zs[2], ws[0])]
            products += [(zs[1], ws[1]), (zs[2], ws[1]), (zs[2], w_ref)]
            lanes = []
            for left, right in products:
                for k in range(comps):
                    lanes.append(jnp.sum(left[k] * right[k], axis=0, keepdims=True))
            while len(lanes) < 32:
                lanes.append(jnp.zeros((1, size), F32))
            quarter = lax.broadcasted_iota(jnp.int32, (8, size), 1) // 32
            folded = jnp.zeros((8, size), F32)
            for q in range(4):
                part = jnp.concatenate(lanes[q * 8 : q * 8 + 8], axis=0)
                part = part + pltpu.roll(part, 64, 1)
                part = part + pltpu.roll(part, 32, 1)
                folded = jnp.where(quarter == q, part, folded)
            for j in range(gram_ref.shape[0]):
                gram_ref[j] = folded
            return
        put_rows(rows_ref, 0, applied)

        def pre_step(c, carry):
            wait_for(remote // chunk + c)
            results = []
            for j in range(0, chunk, 2):
                n = c * chunk + j
                results.extend(
                    pair_dot(
                        rows_at(rows_ref, n),
                        rows_at(rows_ref, n + 1),
                        tiles[remote + n],
                        tiles[remote + n + 1],
                    )
                )
            for j in range(chunk):
                acc_ref[pl.ds(pl.multiple_of((c * chunk + j) * 8, 8), 8), :] = results[j]
            return carry

        lax.fori_loop(0, nb // chunk, pre_step, 0)
        smoothed = take_rows(acc_ref, comps, nb)
        for k in range(comps):
            z_ref[k] = smoothed[k] if first else smoothed[k] - SHIFT * v_ref[k]
        write_sends(dom_rows, sub_rows, z_ref, outs)

    def finish_kernel(parts, *refs):
        x_ref, r_ref, z0, z1, z2, w0, w1, w2, sol_ref, res_ref = refs
        total = jnp.sum(parts[...], axis=0)
        quarter = lax.broadcasted_iota(jnp.int32, (8, size), 1) // 32
        sums = [
            jnp.sum(jnp.where(quarter == q, total, 0.0), axis=1, keepdims=True) for q in range(4)
        ]

        def entry(p, k):
            m = p * comps + k
            return sums[m // 8][m % 8 : m % 8 + 1, :]

        for k in range(comps):
            g0, g1, g2, a00, a01, a02, a11, a12, a22 = [entry(p, k) for p in range(9)]
            l1 = a01 / a00
            l2 = a02 / a00
            d1 = a11 - l1 * a01
            e = a12 - l1 * a02
            m2 = e / d1
            d2 = a22 - l2 * a02 - m2 * e
            y1 = g1 - l1 * g0
            y2 = g2 - l2 * g0 - m2 * y1
            c2 = y2 / d2
            c1 = y1 / d1 - m2 * c2
            c0 = g0 / a00 - l1 * c1 - l2 * c2
            sol = x_ref[k] + c0 * z0[k] + c1 * z1[k] + c2 * z2[k]
            res = r_ref[k] - c0 * w0[k] - c1 * w1[k] - c2 * w2[k]
            for n in range(nb):
                sol_ref[k : k + 1, n * size : (n + 1) * size] = sol[n : n + 1]
                res_ref[k : k + 1, n * size : (n + 1) * size] = res[n : n + 1]

    acc = jax.ShapeDtypeStruct((nb * 8, size), F32)
    send_call = pl.pallas_call(
        send_kernel,
        out_shape=[field] + sends,
        in_specs=[SMEM, SMEM, VMEM],
        out_specs=[VMEM] * (1 + len(sends)),
    )
    local_call = pl.pallas_call(
        local_kernel,
        out_shape=acc,
        in_specs=[SMEM, SMEM, SMEM, ANY, ANY],
        out_specs=VMEM,
        scratch_shapes=[
            pltpu.VMEM((comps, nb, size), F32),
            pltpu.VMEM((lt, size, size), F32),
            pltpu.VMEM((nb * 8, size), F32),
            pltpu.SemaphoreType.DMA((lt // chunk,)),
            pltpu.SemaphoreType.DMA,
        ],
    )

    def remote_call(first, last):
        held = remote if last else remote + nb
        specs = [SMEM] * 6 + [ANY] * (3 + len(sends) + 2)
        if last:
            specs += [VMEM] * (2 * ITERS)
            outs = [field, jax.ShapeDtypeStruct((shape["devices"], 8, size), F32)]
        else:
            specs += [ANY]
            outs = [field, field] + sends
        return pl.pallas_call(
            lambda *refs: remote_kernel(first, last, *refs),
            out_shape=outs,
            in_specs=specs,
            out_specs=[VMEM] * len(outs),
            scratch_shapes=[
                pltpu.VMEM((held, size, size), F32),
                pltpu.VMEM((max(slots, nb) * 8, size), F32),
                pltpu.VMEM((nb * 8, size), F32),
                pltpu.VMEM((comps, nb, size), F32),
                pltpu.VMEM((nb, size), F32),
                pltpu.VMEM((bits, comps, sd, size), F32),
                pltpu.VMEM((turns, comps, ss, size), F32),
                pltpu.SemaphoreType.DMA((held // chunk,)),
                pltpu.SemaphoreType.DMA((len(sends) + 3,)),
            ],
        )

    flat = jax.ShapeDtypeStruct((comps, nb * size), F32)
    finish_call = pl.pallas_call(
        finish_kernel, out_shape=[flat, flat], in_specs=[VMEM] * 9, out_specs=[VMEM, VMEM]
    )
    return send_call, local_call, remote_call, finish_call


def on_device(
    positions,
    mass,
    local_tiles,
    local_rows,
    local_cols,
    live_tiles,
    dom_tiles,
    dom_cols,
    dom_slots,
    dom_rows,
    sub_tiles,
    sub_cols,
    sub_slots,
    sub_rows,
    precond,
):
    count_dom = lax.axis_size("dom")
    count_sub = lax.axis_size("sub")
    nb, size = precond.shape[0], precond.shape[1]
    comps = positions.shape[0]
    sd = dom_rows.shape[0] // count_dom
    ss = sub_rows.shape[0] // count_sub
    bits = (count_dom - 1).bit_length()
    turns = count_sub - 1
    send_call, local_call, remote_call, finish_call = make_calls(
        dict(
            nb=nb,
            size=size,
            comps=comps,
            lt=local_tiles.shape[0],
            ifd=dom_tiles.shape[0],
            ifs=sub_tiles.shape[0],
            sd=sd,
            ss=ss,
            bits=bits,
            turns=turns,
            devices=count_dom * count_sub,
        )
    )
    dom_pairs = [[(a, a ^ (1 << j)) for a in range(count_dom)] for j in range(bits)]
    sub_pairs = [[(b, (b + o) % count_sub) for b in range(count_sub)] for o in range(1, count_sub)]

    def exchange(sends):
        moved = [lax.ppermute(sends[j], "dom", dom_pairs[j]) for j in range(bits)]
        moved += [lax.ppermute(sends[bits + o], "sub", sub_pairs[o]) for o in range(turns)]
        return moved

    weights = mass.reshape(nb, size)
    x, *sends = send_call(dom_rows, sub_rows, positions)
    routes = (dom_slots, dom_cols, sub_slots, sub_cols, dom_rows, sub_rows)
    v = x
    zs, ws = [], []
    for phase in range(ITERS + 1):
        arrived = exchange(sends)
        acc = local_call(local_rows, local_cols, live_tiles, v, local_tiles)
        first, last = phase == 0, phase == ITERS
        held = (*routes, v, weights, acc, *arrived, dom_tiles, sub_tiles)
        if not last:
            w, z, *sends = remote_call(first, last)(*held, precond)
            ws.append(w)
            zs.append(z)
            v = z
        else:
            w, gram = remote_call(first, last)(*held, ws[0], *zs, *ws[1:])
            ws.append(w)
    parts = lax.all_to_all(gram, ("dom", "sub"), 0, 0)
    return tuple(finish_call(parts, x, ws[0], *zs, *ws[1:]))


def solution(mesh):
    both = ("dom", "sub")
    flat, tiles = P(both), P(both, None, None)
    placed = (
        P(None, both),
        flat,
        tiles,
        flat,
        flat,
        flat,
        tiles,
        flat,
        flat,
        flat,
        tiles,
        flat,
        flat,
        flat,
        tiles,
    )
    return jax.shard_map(
        on_device,
        mesh=mesh,
        in_specs=placed,
        out_specs=(P(None, both), P(None, both)),
        check_vma=False,
    )
```

```python
import math

import jax
import jax.numpy as jnp
from jax import lax
from jax.experimental import pallas as pl
from jax.experimental.pallas import tpu as pltpu
from jax.sharding import PartitionSpec as P

ITERS = 3
SHIFT = 1.0
F32 = jnp.float32
BF16 = jnp.bfloat16


VMEM = pl.BlockSpec(memory_space=pltpu.VMEM)
SMEM = pl.BlockSpec(memory_space=pltpu.SMEM)
ANY = pl.BlockSpec(memory_space=pl.ANY)


def keep(values):
    return [pltpu.with_memory_space_constraint(value, pltpu.VMEM) for value in values]


def pair_dot(left_a, left_b, tile_a, tile_b):
    lhs = jnp.concatenate([left_a, left_b], axis=0).astype(BF16)
    lhs = jnp.concatenate([lhs, lhs], axis=1)
    both = jnp.concatenate([tile_a, tile_b], axis=1)
    high = both.astype(BF16)
    low = (both - high.astype(F32)).astype(BF16)
    out = jnp.dot(lhs, jnp.concatenate([high, low], axis=0), preferred_element_type=F32)
    size = tile_a.shape[1]
    return out[0:8, 0:size], out[8:16, size : 2 * size]


def put_rows(rows_ref, start, planes):
    components = len(planes)
    count = planes[0].shape[0]
    for k, plane in enumerate(planes):
        high = plane.astype(BF16).astype(F32)
        rows_ref[pl.ds(start * 8 + k, count, stride=8), :] = high
        rows_ref[pl.ds(start * 8 + components + k, count, stride=8), :] = plane - high
    for k in range(2 * components, 8):
        rows_ref[pl.ds(start * 8 + k, count, stride=8), :] = jnp.zeros(planes[0].shape, F32)


def take_rows(rows_ref, components, count):
    return [
        rows_ref[pl.ds(k, count, stride=8), :] + rows_ref[pl.ds(components + k, count, stride=8), :]
        for k in range(components)
    ]


def rows_at(ref, index):
    return ref[pl.ds(pl.multiple_of(index * 8, 8), 8), :]


def make_calls(shape):
    nb, size, comps = shape["nb"], shape["size"], shape["comps"]
    lt, ifd, ifs = shape["lt"], shape["ifd"], shape["ifs"]
    sd, ss, bits, turns = shape["sd"], shape["ss"], shape["bits"], shape["turns"]
    field = pltpu.VMEM((comps, nb, size), F32)
    sends = [pltpu.VMEM((comps, sd, size), F32)] * bits
    sends += [pltpu.VMEM((comps, ss, size), F32)] * turns
    slots = bits * sd + turns * ss
    remote = ifd + ifs
    width = bits * sd

    def dom_source(slot, mine):
        flipped = (slot // sd) ^ mine
        which = sum((flipped >= (1 << j)).astype(jnp.int32) for j in range(1, bits))
        return which * sd + slot % sd

    def sub_source(slot, mine):
        behind = (mine - slot // ss + turns + 1) % (turns + 1)
        return width + (behind - 1) * ss + slot % ss

    chunk = math.gcd(math.gcd(lt, ifd), math.gcd(math.gcd(ifs, nb), 16))

    def write_sends(dom_rows, sub_rows, v_ref, outs):
        mine_dom, mine_sub = lax.axis_index("dom"), lax.axis_index("sub")
        for j, out in enumerate(outs):
            if j < bits:
                rows, base = dom_rows, (mine_dom ^ (1 << j)) * sd
            else:
                rows, base = sub_rows, (mine_sub + (j - bits + 1)) % (turns + 1) * ss
            for s in range(out.shape[1]):
                row = rows[base + s]
                for k in range(comps):
                    out[k, pl.ds(s, 1), :] = v_ref[k, pl.ds(row, 1), :]

    def send_kernel(dom_rows, sub_rows, x_ref, v_ref, *outs):
        for n in range(nb):
            block = x_ref[:, n * size : (n + 1) * size]
            for k in range(comps):
                v_ref[k, n : n + 1, :] = block[k : k + 1]
        write_sends(dom_rows, sub_rows, v_ref, outs)

    def local_kernel(rows, cols, live, v_ref, tiles_hbm, acc_ref, tiles, rows_ref, sems):
        copies = [
            pltpu.make_async_copy(
                tiles_hbm.at[pl.ds(c * chunk, chunk)], tiles.at[pl.ds(c * chunk, chunk)], sems.at[c]
            )
            for c in range(lt // chunk)
        ]
        for copy in copies:
            copy.start()
        put_rows(rows_ref, 0, [v_ref[k] for k in range(comps)])
        acc_ref[...] = jnp.zeros(acc_ref.shape, F32)

        def step(c, carry):
            pltpu.make_async_copy(
                tiles_hbm.at[pl.ds(c * chunk, chunk)], tiles.at[pl.ds(c * chunk, chunk)], sems.at[c]
            ).wait()
            results = []
            for j in range(0, chunk, 2):
                t = c * chunk + j
                results.extend(
                    pair_dot(
                        rows_at(rows_ref, rows[t]),
                        rows_at(rows_ref, rows[t + 1]),
                        tiles[t],
                        tiles[t + 1],
                    )
                )
            for j in range(chunk):
                t = c * chunk + j
                used = t < live[0]
                place = pl.ds(pl.multiple_of(cols[t] * 8, 8), 8)
                acc_ref[place, :] += jnp.where(used, results[j], 0.0)
            return carry

        lax.fori_loop(0, lt // chunk, step, 0)

    def remote_kernel(first, last, *refs):
        dom_slots, dom_cols, sub_slots, sub_cols, dom_rows, sub_rows = refs[:6]
        v_ref, mass_hbm, start_acc = refs[6:9]
        refs = refs[9:]
        arrived, refs = refs[: bits + turns], refs[bits + turns :]
        dom_hbm, sub_hbm, refs = refs[0], refs[1], refs[2:]
        if not last:
            pre_hbm, w_ref, z_ref, refs = refs[0], refs[1], refs[2], refs[3:]
            outs, refs = refs[: bits + turns], refs[bits + turns :]
            sources = ((dom_hbm, ifd), (sub_hbm, ifs), (pre_hbm, nb))
        else:
            past, refs = refs[: 2 * ITERS], refs[2 * ITERS :]
            w_ref, gram_ref, refs = refs[0], refs[1], refs[2:]
            sources = ((dom_hbm, ifd), (sub_hbm, ifs))
        tiles, rows_ref, acc_ref, mass_ref, sems, mass_sem = refs
        mass_copy = pltpu.make_async_copy(mass_hbm, mass_ref, mass_sem)
        base = 0
        for source, count in sources:
            for c in range(count // chunk):
                pltpu.make_async_copy(
                    source.at[pl.ds(c * chunk, chunk)],
                    tiles.at[pl.ds(base + c * chunk, chunk)],
                    sems.at[(base // chunk) + c],
                ).start()
            base += count
        mass_copy.start()
        start = 0
        for ref in arrived:
            put_rows(rows_ref, start, [ref[k] for k in range(comps)])
            start += ref.shape[1]
        acc_ref[...] = start_acc[...]

        def wait_for(c):
            pltpu.make_async_copy(
                dom_hbm.at[pl.ds(0, chunk)], tiles.at[pl.ds(c * chunk, chunk)], sems.at[c]
            ).wait()

        def apply_tiles(base, count, slots_ref, cols_ref, source, mine):
            def step(c, carry):
                wait_for(base // chunk + c)
                results = []
                for j in range(0, chunk, 2):
                    t = c * chunk + j
                    results.extend(
                        pair_dot(
                            rows_at(rows_ref, source(slots_ref[t], mine)),
                            rows_at(rows_ref, source(slots_ref[t + 1], mine)),
                            tiles[base + t],
                            tiles[base + t + 1],
                        )
                    )
                for j in range(chunk):
                    place = pl.ds(pl.multiple_of(cols_ref[c * chunk + j] * 8, 8), 8)
                    acc_ref[place, :] += results[j]
                return carry

            lax.fori_loop(0, count // chunk, step, 0)

        apply_tiles(0, ifd, dom_slots, dom_cols, dom_source, lax.axis_index("dom"))
        apply_tiles(ifd, ifs, sub_slots, sub_cols, sub_source, lax.axis_index("sub"))
        mass_copy.wait()
        summed = take_rows(acc_ref, comps, nb)
        if first:
            applied = [-x for x in summed]
        else:
            applied = [mass_ref[...] * v_ref[k] + summed[k] for k in range(comps)]
        for k in range(comps):
            w_ref[k] = applied[k]
        if last:
            start_res, zs, ws = past[0], past[1:4], past[4:6]
            products = [(zs[i], start_res) for i in range(ITERS)]
            products += [(zs[0], ws[0]), (zs[1], ws[0]), (zs[2], ws[0])]
            products += [(zs[1], ws[1]), (zs[2], ws[1]), (zs[2], w_ref)]
            lanes = []
            for left, right in products:
                for k in range(comps):
                    lanes.append(jnp.sum(left[k] * right[k], axis=0, keepdims=True))
            while len(lanes) < 32:
                lanes.append(jnp.zeros((1, size), F32))
            quarter = lax.broadcasted_iota(jnp.int32, (8, size), 1) // 32
            folded = jnp.zeros((8, size), F32)
            for q in range(4):
                part = jnp.concatenate(lanes[q * 8 : q * 8 + 8], axis=0)
                part = part + pltpu.roll(part, 64, 1)
                part = part + pltpu.roll(part, 32, 1)
                folded = jnp.where(quarter == q, part, folded)
            for j in range(gram_ref.shape[0]):
                gram_ref[j] = folded
            return
        put_rows(rows_ref, 0, applied)

        def pre_step(c, carry):
            wait_for(remote // chunk + c)
            results = []
            for j in range(0, chunk, 2):
                n = c * chunk + j
                results.extend(
                    pair_dot(
                        rows_at(rows_ref, n),
                        rows_at(rows_ref, n + 1),
                        tiles[remote + n],
                        tiles[remote + n + 1],
                    )
                )
            for j in range(chunk):
                acc_ref[pl.ds(pl.multiple_of((c * chunk + j) * 8, 8), 8), :] = results[j]
            return carry

        lax.fori_loop(0, nb // chunk, pre_step, 0)
        smoothed = take_rows(acc_ref, comps, nb)
        for k in range(comps):
            z_ref[k] = smoothed[k] if first else smoothed[k] - SHIFT * v_ref[k]
        write_sends(dom_rows, sub_rows, z_ref, outs)

    def finish_kernel(parts, *refs):
        x_ref, r_ref, z0, z1, z2, w0, w1, w2, sol_ref, res_ref = refs
        total = jnp.sum(parts[...], axis=0)
        quarter = lax.broadcasted_iota(jnp.int32, (8, size), 1) // 32
        sums = [
            jnp.sum(jnp.where(quarter == q, total, 0.0), axis=1, keepdims=True) for q in range(4)
        ]

        def entry(p, k):
            m = p * comps + k
            return sums[m // 8][m % 8 : m % 8 + 1, :]

        for k in range(comps):
            g0, g1, g2, a00, a01, a02, a11, a12, a22 = [entry(p, k) for p in range(9)]
            l1 = a01 / a00
            l2 = a02 / a00
            d1 = a11 - l1 * a01
            e = a12 - l1 * a02
            m2 = e / d1
            d2 = a22 - l2 * a02 - m2 * e
            y1 = g1 - l1 * g0
            y2 = g2 - l2 * g0 - m2 * y1
            c2 = y2 / d2
            c1 = y1 / d1 - m2 * c2
            c0 = g0 / a00 - l1 * c1 - l2 * c2
            sol = x_ref[k] + c0 * z0[k] + c1 * z1[k] + c2 * z2[k]
            res = r_ref[k] - c0 * w0[k] - c1 * w1[k] - c2 * w2[k]
            for n in range(nb):
                sol_ref[k : k + 1, n * size : (n + 1) * size] = sol[n : n + 1]
                res_ref[k : k + 1, n * size : (n + 1) * size] = res[n : n + 1]

    acc = pltpu.VMEM((nb * 8, size), F32)
    send_call = pl.pallas_call(
        send_kernel,
        out_shape=[field] + sends,
        in_specs=[SMEM, SMEM, VMEM],
        out_specs=[VMEM] * (1 + len(sends)),
    )
    local_call = pl.pallas_call(
        local_kernel,
        out_shape=acc,
        in_specs=[SMEM, SMEM, SMEM, VMEM, ANY],
        out_specs=VMEM,
        scratch_shapes=[
            pltpu.VMEM((lt, size, size), F32),
            pltpu.VMEM((nb * 8, size), F32),
            pltpu.SemaphoreType.DMA((lt // chunk,)),
        ],
    )

    def remote_call(first, last):
        held = remote if last else remote + nb
        specs = [SMEM] * 6 + [VMEM, ANY, VMEM] + [VMEM] * len(sends) + [ANY] * 2
        if last:
            specs += [VMEM] * (2 * ITERS)
            outs = [field, pltpu.VMEM((shape["devices"], 8, size), F32)]
        else:
            specs += [ANY]
            outs = [field, field] + sends
        return pl.pallas_call(
            lambda *refs: remote_kernel(first, last, *refs),
            out_shape=outs,
            in_specs=specs,
            out_specs=[VMEM] * len(outs),
            scratch_shapes=[
                pltpu.VMEM((held, size, size), F32),
                pltpu.VMEM((max(slots, nb) * 8, size), F32),
                pltpu.VMEM((nb * 8, size), F32),
                pltpu.VMEM((nb, size), F32),
                pltpu.SemaphoreType.DMA((held // chunk,)),
                pltpu.SemaphoreType.DMA,
            ],
        )

    flat = jax.ShapeDtypeStruct((comps, nb * size), F32)
    finish_call = pl.pallas_call(
        finish_kernel, out_shape=[flat, flat], in_specs=[VMEM] * 9, out_specs=[VMEM, VMEM]
    )
    return send_call, local_call, remote_call, finish_call


def on_device(
    positions,
    mass,
    local_tiles,
    local_rows,
    local_cols,
    live_tiles,
    dom_tiles,
    dom_cols,
    dom_slots,
    dom_rows,
    sub_tiles,
    sub_cols,
    sub_slots,
    sub_rows,
    precond,
):
    count_dom = lax.axis_size("dom")
    count_sub = lax.axis_size("sub")
    nb, size = precond.shape[0], precond.shape[1]
    comps = positions.shape[0]
    sd = dom_rows.shape[0] // count_dom
    ss = sub_rows.shape[0] // count_sub
    bits = (count_dom - 1).bit_length()
    turns = count_sub - 1
    send_call, local_call, remote_call, finish_call = make_calls(
        dict(
            nb=nb,
            size=size,
            comps=comps,
            lt=local_tiles.shape[0],
            ifd=dom_tiles.shape[0],
            ifs=sub_tiles.shape[0],
            sd=sd,
            ss=ss,
            bits=bits,
            turns=turns,
            devices=count_dom * count_sub,
        )
    )
    dom_pairs = [[(a, a ^ (1 << j)) for a in range(count_dom)] for j in range(bits)]
    sub_pairs = [[(b, (b + o) % count_sub) for b in range(count_sub)] for o in range(1, count_sub)]

    def exchange(sends):
        moved = [lax.ppermute(sends[j], "dom", dom_pairs[j]) for j in range(bits)]
        moved += [lax.ppermute(sends[bits + o], "sub", sub_pairs[o]) for o in range(turns)]
        return keep(moved)

    weights = mass.reshape(nb, size)
    x, *sends = keep(send_call(dom_rows, sub_rows, positions))
    routes = (dom_slots, dom_cols, sub_slots, sub_cols, dom_rows, sub_rows)
    v = x
    zs, ws = [], []
    for phase in range(ITERS + 1):
        arrived = exchange(sends)
        (acc,) = keep([local_call(local_rows, local_cols, live_tiles, v, local_tiles)])
        first, last = phase == 0, phase == ITERS
        held = (*routes, v, weights, acc, *arrived, dom_tiles, sub_tiles)
        if not last:
            w, z, *sends = keep(remote_call(first, last)(*held, precond))
            ws.append(w)
            zs.append(z)
            v = z
        else:
            w, gram = keep(remote_call(first, last)(*held, ws[0], *zs, *ws[1:]))
            ws.append(w)
    parts = lax.all_to_all(gram, ("dom", "sub"), 0, 0)
    return tuple(finish_call(parts, x, ws[0], *zs, *ws[1:]))


def solution(mesh):
    both = ("dom", "sub")
    flat, tiles = P(both), P(both, None, None)
    placed = (
        P(None, both),
        flat,
        tiles,
        flat,
        flat,
        flat,
        tiles,
        flat,
        flat,
        flat,
        tiles,
        flat,
        flat,
        flat,
        tiles,
    )
    return jax.shard_map(
        on_device,
        mesh=mesh,
        in_specs=placed,
        out_specs=(P(None, both), P(None, both)),
        check_vma=False,
    )
```
